32 devices in a mesh: sph: 32 (over z, y, x, core).
Axes of the slice: x: 2, y: 2, z: 4, core: 2. Of those that a mesh axis runs over, the one named last changes fastest.
Arguments:
- right_side: float32 [512, 2, 336], P('sph'), may hold values from -8 to 8
- positions: float32 [3, 512], P(None, 'sph'), may hold values from -0.1 to 15.1, as said below
- sphere_radii: float32 [512], P('sph'), may hold values from 0.2 to 0.35
- azimuths: float32 [512], P('sph'), may hold values from -3.1416 to 3.1416
- pair_flags: int32 [512, 512], P('sph'), may hold values from 0 to 2, as said below
- pair_counts: int32 [512], P('sph'), may hold values from 1 to 511, as said below
- tilt_matrix: float32 [336, 336], replicated, may hold values from -1 to 1
- axial_terms: float32 [8, 336, 336], replicated, may hold values from -1 to 1
Outputs:
- solution: float32 [512, 2, 336], P('sph')
- residual: float32 [512, 2, 336], P('sph')
- direction: float32 [512, 2, 336], P('sph')
The draws below stay inside these ranges and needn't reach their ends.
Inputs may be any that keep to these rules, and one draw needn't show every extreme that they name: pair_flags is symmetric and zero on the diagonal. pair_counts[i] is the number of j with pair_flags[i, j] != 0; one sphere is linked to every other. `positions`: any two sphere centres are at least 0.8 apart.
All inputs are finite; a program needn't handle non-finite values.
Results may differ from the reference program's by a relative error of at most 0.0003.
Values sent between devices are 32-bit elements; how exact they have to be, the bound alone decides.
A program may use at most 64 MiB of HBM per device.

```python
import math
import jax
import jax.numpy as jnp
import numpy as np
from jax import lax

SPH_DEV = 16
DEG = 12
HALF = 168
C = 336
TERMS = 8
SPHERES = 512
N_SPH = 32


def lattice_cells(total):
    sphere_ids = jnp.arange(total, dtype=jnp.int32)
    return jnp.stack([sphere_ids % 16, sphere_ids // 16 % 16, sphere_ids // 256])


def flag_table(key):
    cells = lattice_cells(SPHERES)
    spread = jnp.zeros((SPHERES, SPHERES), jnp.int32)
    for axis_index in range(3):
        spread = jnp.maximum(spread, jnp.abs(cells[axis_index][:, None] - cells[axis_index][None, :]))
    coin_bits = jax.random.randint(jax.random.fold_in(key, 11), (SPHERES, SPHERES), 0, 4)
    hub_sphere = jax.random.randint(jax.random.fold_in(key, 13), (), 0, SPHERES)
    row_ids = jnp.arange(SPHERES, dtype=jnp.int32)[:, None]
    col_ids = jnp.arange(SPHERES, dtype=jnp.int32)[None, :]
    shared_bits = jnp.where(row_ids < col_ids, coin_bits, coin_bits.T)
    hub_pair = (row_ids == hub_sphere) | (col_ids == hub_sphere)
    dropped = (shared_bits == 0) & jnp.logical_not(hub_pair) | (row_ids == col_ids)
    classes = jnp.where(spread <= 2, 1, 2)
    return jnp.where(dropped, 0, classes).astype(jnp.int32)


def draw_positions(key, part):
    cells = lattice_cells(SPHERES).astype(jnp.float32)
    jitter = jax.random.uniform(key, (3, SPHERES), jnp.float32, -0.1, 0.1)
    return cells + jitter


def draw_pair_flags(key, part):
    return flag_table(key)


def draw_pair_counts(key, part):
    return jnp.sum((flag_table(key) != 0).astype(jnp.int32), axis=1)


def scaled_matrix(key, shape, fan_width):
    values = jnp.clip(jax.random.normal(key, shape, jnp.float32), -4.0, 4.0) / math.sqrt(float(fan_width))
    return values


def draw_tilt_matrix(key, part):
    return scaled_matrix(jax.random.fold_in(key, 31), (C, C), C)


def draw_axial_terms(key, part):
    return scaled_matrix(jax.random.fold_in(key, 37), (TERMS, C, C), C)


def draw_azimuths(key, part):
    return jax.random.uniform(jax.random.fold_in(key, 41), (SPHERES,), jnp.float32, -math.pi, math.pi)


def orders_list():
    return np.concatenate([np.arange(-degree, degree + 1) for degree in range(1, DEG + 1)]).astype(np.float32)


def turn_rows(vector, azimuth, handed):
    phases = azimuth[:, None] * jnp.asarray(orders_list())[None, :]
    cosine = jnp.cos(phases)[:, None, :]
    sine_part = handed * jnp.sin(phases)[:, None, :]
    real_part = vector[..., :HALF]
    imag_part = vector[..., HALF:]
    return jnp.concatenate([cosine * real_part - sine_part * imag_part, sine_part * real_part + cosine * imag_part], axis=-1)


def leading_image(rough, key, part):
    centres = draw_positions(key, part)
    flags = flag_table(key)
    counts = jnp.sum((flags != 0).astype(jnp.float32), axis=1)
    angles = draw_azimuths(key, part)
    tilt = draw_tilt_matrix(key, part)
    axial_zero = draw_axial_terms(key, part)[0]
    delta = centres[:, :, None] - centres[:, None, :]
    distance = jnp.sqrt(jnp.sum(delta * delta, axis=0))
    weights = 0.25 * jnp.cos(2.5 * distance) * (flags != 0).astype(jnp.float32)
    framed = jnp.einsum('spk,kl->spl', turn_rows(rough, angles, 1.0), tilt, precision=lax.Precision.HIGHEST)
    summed = jnp.einsum('ij,jpk->ipk', weights, framed, precision=lax.Precision.HIGHEST)
    moved = jnp.einsum('ipk,kl->ipl', summed, axial_zero, precision=lax.Precision.HIGHEST)
    unturned = jnp.einsum('ipl,kl->ipk', moved, tilt, precision=lax.Precision.HIGHEST)
    unturned = unturned / jnp.sqrt(1.0 + counts)[:, None, None]
    return turn_rows(unturned, angles, -1.0)


def draw_right_side(key, part):
    rough = jnp.clip(jax.random.normal(jax.random.fold_in(key, 21), (SPHERES, 2, C), jnp.float32), -4.0, 4.0)
    return jnp.clip(rough + 2.0 * leading_image(rough, key, part), -8.0, 8.0)


def block_scale(own_key, extent, shards, least, top_value):
    level = 1.0
    for position, blocks in shards:
        steps = jax.random.uniform(jax.random.fold_in(jax.random.fold_in(own_key, 6), position), (blocks,), jnp.float32, least / len(shards), top_value / len(shards))
        level = level * jnp.repeat(jnp.exp(steps), extent[position] // blocks).reshape((-1,) + (1,) * (len(extent) - 1 - position))
    return level


def setup_inputs(seed: int = 0) -> dict:
    keys = jax.random.split(jax.random.key(seed), 9)
    return {
        "right_side": draw_right_side(jax.random.fold_in(keys[8], 71), 0),
        "positions": draw_positions(jax.random.fold_in(keys[8], 71), 0),
        "sphere_radii": jnp.clip(0.2 + 0.14999999 * jax.random.uniform(keys[2], (SPHERES,), jnp.float32) ** block_scale(keys[2], (SPHERES,), ((0, 32),), -0.2, 0.2), 0.2, 0.35),
        "azimuths": draw_azimuths(jax.random.fold_in(keys[8], 71), 0),
        "pair_flags": draw_pair_flags(jax.random.fold_in(keys[8], 71), 0),
        "pair_counts": draw_pair_counts(jax.random.fold_in(keys[8], 71), 0),
        "tilt_matrix": draw_tilt_matrix(jax.random.fold_in(keys[8], 71), 0),
        "axial_terms": draw_axial_terms(jax.random.fold_in(keys[8], 71), 0),
    }


coupling = 0.25
wavenum = 2.5
phase_step = 0.9
dist_floor = 0.8

def orders_table():
    return np.concatenate([np.arange(-degree, degree + 1) for degree in range(1, DEG + 1)]).astype(np.float32)

def rotate_z(vector, azimuth, handed):
    half_len = vector.shape[-1] // 2
    phases = azimuth[:, None] * jnp.asarray(orders_table())[None, :]
    cosine = jnp.cos(phases)[:, None, :]
    sine_part = handed * jnp.sin(phases)[:, None, :]
    real_part = vector[..., :half_len]
    imag_part = vector[..., half_len:]
    return jnp.concatenate([cosine * real_part - sine_part * imag_part, sine_part * real_part + cosine * imag_part], axis=-1)

def pair_weights(flag_block, geo_rows, geo_cols):
    delta_x = geo_rows[0][:, None] - geo_cols[0][None, :]
    delta_y = geo_rows[1][:, None] - geo_cols[1][None, :]
    delta_z = geo_rows[2][:, None] - geo_cols[2][None, :]
    distance = jnp.sqrt(delta_x * delta_x + delta_y * delta_y + delta_z * delta_z)
    size_ratio = (geo_rows[3][:, None] + geo_cols[3][None, :]) / jnp.maximum(distance, dist_floor)
    linked = (flag_block != 0).astype(distance.dtype)
    nearby = (flag_block == 1).astype(distance.dtype)
    ratio_power = jnp.ones_like(distance)
    weights = []
    for term_index in range(TERMS):
        selector = linked if term_index == 0 else nearby
        weights.append(coupling * ratio_power * jnp.cos(wavenum * distance + phase_step * term_index) * selector)
        ratio_power = ratio_power * size_ratio
    return jnp.stack(weights)

def to_frame(vector, azimuths, tilt_matrix):
    return jnp.einsum('spk,kl->spl', rotate_z(vector, azimuths, 1.0), tilt_matrix, precision=lax.Precision.HIGHEST)

def from_frame(coupled, azimuths, tilt_matrix, pair_counts):
    unturned = jnp.einsum('spl,kl->spk', coupled, tilt_matrix, precision=lax.Precision.HIGHEST)
    inverse_root = 1.0 / jnp.sqrt(1.0 + pair_counts.astype(jnp.float32))
    return rotate_z(unturned * inverse_root[:, None, None], azimuths, -1.0)

def operate(vector, azimuths, geometry, pair_flags, pair_counts, tilt_matrix, axial_terms):
    framed = to_frame(vector, azimuths, tilt_matrix)
    flat_rows = framed.reshape(SPHERES, -1)

    def target_block(block_index):
        row_start = block_index * SPH_DEV
        geo_rows = lax.dynamic_slice_in_dim(geometry, row_start, SPH_DEV, 1)
        flag_block = lax.dynamic_slice_in_dim(pair_flags, row_start, SPH_DEV, 0)
        weights = pair_weights(flag_block, geo_rows, geometry)
        gathered = jnp.einsum('mtj,jk->mtk', weights, flat_rows, precision=lax.Precision.HIGHEST)
        gathered = gathered.reshape(TERMS, SPH_DEV, 2, -1)
        return jnp.einsum('mtpk,mkl->tpl', gathered, axial_terms, precision=lax.Precision.HIGHEST)
    coupled = lax.map(target_block, jnp.arange(N_SPH, dtype=jnp.int32)).reshape(vector.shape)
    return vector - from_frame(coupled, azimuths, tilt_matrix, pair_counts)

def reference(right_side, positions, sphere_radii, azimuths, pair_flags, pair_counts, tilt_matrix, axial_terms):
    geometry = jnp.concatenate([positions, sphere_radii[None, :]], axis=0)

    def apply_op(vector):
        return operate(vector, azimuths, geometry, pair_flags, pair_counts, tilt_matrix, axial_terms)
    rho_start = jnp.sum(right_side * right_side)
    image_p = apply_op(right_side)
    step_alpha = rho_start / jnp.sum(right_side * image_p)
    half_step = right_side - step_alpha * image_p
    half_image = apply_op(half_step)
    step_omega = jnp.sum(half_image * half_step) / jnp.sum(half_image * half_image)
    solution = step_alpha * right_side + step_omega * half_step
    residual = half_step - step_omega * half_image
    rho_next = jnp.sum(right_side * residual)
    step_beta = rho_next / rho_start * (step_alpha / step_omega)
    direction = residual + step_beta * (right_side - step_omega * image_p)
    return (solution, residual, direction)
```

```python
import functools

import jax
import jax.numpy as jnp
import numpy as np
from jax import lax
from jax.experimental import pallas as pl
from jax.experimental.pallas import tpu as pltpu
from jax.sharding import PartitionSpec as P

coupling = 0.25
wavenum = 2.5
phase_step = 0.9
dist_floor = 0.8

LANES = 128
MESH = pl.DeviceIdType.MESH
BF = jnp.bfloat16
F32 = jnp.float32


def orders_table(half):
    degree, orders = 1, []
    while len(orders) < half:
        orders += list(range(-degree, degree + 1))
        degree += 1
    return np.asarray(orders, np.float32)


def split(value):
    high = value.astype(BF)
    return high, (value - high.astype(F32)).astype(BF)


def dot3(high, low, w_high, w_low):
    rows = high.shape[0]
    both = jnp.dot(
        jnp.concatenate([high, low], axis=0), w_high, preferred_element_type=F32
    )
    return (
        both[:rows]
        + both[rows:]
        + jnp.dot(high, w_low, preferred_element_type=F32)
    )


def kernel(
    n, S, C, CP, terms,
    r_ref, pos_ref, rad_ref, az_ref, counts_ref, flags_ref, orders_ref, tilt_ref, axial_ref,
    out_ref, rows_scr,
    own1, own2, buf1, buf2, f_hi, f_lo, w_hi, w_lo, t_hi, t_lo, tt_hi, tt_lo,
    g_raw, g_hi, g_lo, sums, g_sem, send_sem, recv_sem, sum_send, sum_recv,
):
    half = C // 2
    q = n // 8
    me = lax.axis_index("sph")
    core = lax.rem(me, 2)
    x_bit = lax.rem(me // 2, 2)
    y_bit = lax.rem(me // 4, 2)
    other = me + 1 - 2 * core
    x_nb = me + 2 - 4 * x_bit
    y_nb = me + 4 - 8 * y_bit
    near_a = x_nb * (1 - core) + y_nb * core
    near_b = y_nb * (1 - core) + x_nb * core
    diag = x_nb + y_nb - me

    z_at = me // 8

    def flipped(k):
        place, bit = z_at, 1
        while bit <= k:
            if k & bit:
                place = place + bit - 2 * bit * lax.rem(z_at // bit, 2)
            bit *= 2
        return place

    places = [flipped(k) for k in range(q)]
    if q == 4:
        low, high = lax.rem(z_at, 2), z_at // 2
        inner = low + high - 2 * low * high
        swing = inner * (places[3] - places[2])
        places[2], places[3] = places[2] + swing, places[3] - swing

    def shifted(base, k):
        return base + 8 * (places[k] - z_at)

    barrier = pltpu.get_barrier_semaphore()
    peers = [other, x_nb, y_nb, diag] + [shifted(me, k) for k in range(1, q)]
    for peer in peers:
        pl.semaphore_signal(barrier, inc=1, device_id=(peer,), device_id_type=MESH)
    axial_copy = pltpu.make_async_copy(axial_ref, g_raw, g_sem)
    axial_copy.start()

    rows_scr[...] = jnp.zeros_like(rows_scr)
    rows_scr[0:3, 0:S] = pos_ref[...]
    rows_scr[3:4, 0:S] = rad_ref[...]
    rows_scr[4:5, 0:S] = az_ref[...]
    rows_scr[5:6, 0:S] = counts_ref[...].astype(F32)
    cols = rows_scr[...].T[0:S]
    lane = lax.broadcasted_iota(jnp.int32, (S, CP), 1)
    phases = cols[:, 4:5] * orders_ref[...]
    cos_t = jnp.cos(phases)
    sin_t = jnp.sin(phases)
    cos2 = jnp.concatenate([cos_t, cos_t], axis=0)
    sin2 = jnp.concatenate([sin_t, sin_t], axis=0)
    lane2 = jnp.concatenate([lane, lane], axis=0)
    root = 1.0 / jnp.sqrt(1.0 + cols[:, 5:6])
    root2 = jnp.concatenate([root, root], axis=0)

    def swapped(v):
        return jnp.where(
            lane2 < half, -pltpu.roll(v, CP - half, 1), pltpu.roll(v, half, 1)
        )

    t_f32 = tilt_ref[...]
    th, tl = split(t_f32)
    for ref in (t_hi, t_lo, tt_hi, tt_lo):
        ref[...] = jnp.zeros_like(ref)
    t_hi[0:C, 0:C] = th
    t_lo[0:C, 0:C] = tl

    def framed(v):
        turned = cos2 * v + sin2 * swapped(v)
        high, low = split(turned)
        return dot3(high, low, t_hi[...], t_lo[...])

    pad = jnp.zeros((S, CP - C), F32)
    r_vec = jnp.concatenate(
        [
            jnp.concatenate([r_ref[:, 0, :], pad], axis=1),
            jnp.concatenate([r_ref[:, 1, :], pad], axis=1),
        ],
        axis=0,
    )

    def store_block(own, fr, extras):
        second = fr[S:]
        for i, extra in enumerate(extras):
            second = jnp.where(lane == C + i, extra, second)
        own[:, 0:CP] = fr[:S]
        own[:, CP:] = second

    def rows_of(origin):
        return pl.ds(pl.multiple_of(origin * S, S), S)

    def gather(phase, own, buf, fillers):
        sends = []

        def send(slot, k, src, origin, dev):
            copy = pltpu.make_async_remote_copy(
                src_ref=src,
                dst_ref=buf.at[rows_of(origin), :],
                send_sem=send_sem.at[phase, slot, k],
                recv_sem=recv_sem.at[phase, origin],
                device_id=(dev,),
                device_id_type=MESH,
            )
            copy.start()
            sends.append(copy)

        def absorb_value(x, origin):
            high, low = split(x)
            f_hi[rows_of(origin), :] = high
            f_lo[rows_of(origin), :] = low

        def arrive(origin):
            ref = buf.at[rows_of(origin), :]
            pltpu.make_async_remote_copy(
                src_ref=ref, dst_ref=ref,
                send_sem=send_sem.at[phase, 0, 0],
                recv_sem=recv_sem.at[phase, origin],
                device_id=(other,), device_id_type=MESH,
            ).wait_recv()
            return ref

        def absorb(origin):
            absorb_value(buf[rows_of(origin), :], origin)

        fillers = list(fillers)

        def fill():
            if fillers:
                fillers.pop(0)()

        relayed = ()

        def spread(k, ref, origin):
            send(2, k, ref, origin, near_b)
            send(1, k, ref, origin, near_a)
            if k not in relayed:
                send(3, k, ref, origin, diag)
            send(4, k, ref, origin, other)

        def take_a(k):
            origin = shifted(near_a, k)
            ref = arrive(origin)
            if k in relayed:
                send(3, k, ref, origin, near_b)
            send(5, k, ref, origin, other)
            absorb(origin)

        def take(slot, base, k):
            origin = shifted(base, k)
            ref = arrive(origin)
            send(slot, k, ref, origin, other)
            absorb(origin)

        for k in range(1, q):
            send(0, k, own, me, shifted(me, k))
        spread(0, own, me)
        mine = own[...]
        buf[rows_of(me), :] = mine
        absorb_value(mine, me)
        for _ in range(3):
            fill()
        for step in range(1, q + 2):
            if step < q:
                origin = shifted(me, step)
                spread(step, arrive(origin), origin)
                absorb(origin)
                fill()
            if step - 1 < q:
                take_a(step - 1)
                take(6, near_b, step - 1)
                fill()
            if 0 <= step - 2 < q:
                take(7, diag, step - 2)
                fill()
        while fillers:
            fill()
        flip = other - me
        for k in range(q):
            for base in (me, near_b, near_a, diag):
                origin = shifted(base, k) + flip
                arrive(origin)
                absorb(origin)
        return sends

    def apply_op():
        gathered = dot3(w_hi[...], w_lo[...], f_hi[...], f_lo[...])
        x = jnp.concatenate(
            [
                jnp.concatenate(
                    [gathered[m * S : (m + 1) * S, p * CP : (p + 1) * CP] for p in range(2)],
                    axis=0,
                )
                for m in range(terms)
            ],
            axis=1,
        )
        high, low = split(x)
        coupled = dot3(high, low, g_hi[...], g_lo[...])
        high, low = split(coupled)
        unturned = dot3(high, low, tt_hi[...], tt_lo[...]) * root2
        return cos2 * unturned - sin2 * swapped(unturned)

    store_block(own1, framed(r_vec), [cols[:, i : i + 1] for i in range(4)])
    pl.semaphore_wait(barrier, len(peers))

    def fill_tilt():
        h2, l2 = split(t_f32.T)
        tt_hi[0:C, 0:C] = h2
        tt_lo[0:C, 0:C] = l2

    def fill_zero():
        g_hi[...] = jnp.zeros_like(g_hi)
        g_lo[...] = jnp.zeros_like(g_lo)
        axial_copy.wait()

    def fill_axial(m):
        h2, l2 = split(g_raw[m])
        g_hi[m * CP : m * CP + C, 0:C] = h2
        g_lo[m * CP : m * CP + C, 0:C] = l2

    fillers = [fill_tilt, fill_zero] + [
        functools.partial(fill_axial, m) for m in range(terms)
    ]
    sends = gather(0, own1, buf1, fillers)

    geo = buf1[:, 2 * CP - LANES :].T
    at = C - (CP - LANES)
    dx = cols[:, 0:1] - geo[at : at + 1]
    dy = cols[:, 1:2] - geo[at + 1 : at + 2]
    dz = cols[:, 2:3] - geo[at + 2 : at + 3]
    distance = jnp.sqrt(dx * dx + dy * dy + dz * dz)
    ratio = (cols[:, 3:4] + geo[at + 3 : at + 4]) / jnp.maximum(distance, dist_floor)
    flags = flags_ref[...]
    wave = wavenum * distance
    cos_w = coupling * jnp.cos(wave)
    sin_w = coupling * jnp.sin(wave)
    power = jnp.ones_like(distance)
    for m in range(terms):
        turn_c = float(np.cos(phase_step * m))
        turn_s = float(np.sin(phase_step * m))
        keep = (flags != 0) if m == 0 else (flags == 1)
        weight = jnp.where(keep, power * (turn_c * cos_w - turn_s * sin_w), 0.0)
        power = power * ratio
        high, low = split(weight)
        w_hi[m * S : (m + 1) * S, :] = high
        w_lo[m * S : (m + 1) * S, :] = low

    p_vec = r_vec - apply_op()

    def per_sphere(a, b):
        both = jnp.sum(a * b, axis=1, keepdims=True)
        return both[:S] + both[S:]

    store_block(own2, framed(p_vec), [per_sphere(r_vec, r_vec), per_sphere(r_vec, p_vec)])
    sends += gather(1, own2, buf2, [])
    q_vec = p_vec - apply_op()

    starts = jnp.sum(buf2[:, 2 * CP - LANES :], axis=0, keepdims=True)
    rho_start = starts[:, at : at + 1]
    alpha = rho_start / starts[:, at + 1 : at + 2]
    half_step = r_vec - alpha * p_vec
    half_image = p_vec - alpha * q_vec

    def total(a, b):
        return jnp.sum(jnp.sum(a * b, axis=0, keepdims=True), axis=1, keepdims=True)

    lane1 = lax.broadcasted_iota(jnp.int32, (1, LANES), 1)
    row = jnp.zeros((1, LANES), F32)
    pairs = (
        (half_image, half_step),
        (half_image, half_image),
        (r_vec, half_step),
        (r_vec, half_image),
    )
    for i, (a, b) in enumerate(pairs):
        row = jnp.where(lane1 == i, total(a, b), row)
    sums[me] = row

    def sum_copy(k, origin, dev):
        return pltpu.make_async_remote_copy(
            src_ref=sums.at[origin],
            dst_ref=sums.at[origin],
            send_sem=sum_send.at[k],
            recv_sem=sum_recv.at[origin],
            device_id=(dev,),
            device_id_type=MESH,
        )

    @pl.loop(1, n)
    def _(k):
        sum_copy(k, me, lax.rem(me + k, n)).start()

    for copy in sends:
        copy.wait_send()

    @pl.loop(1, n)
    def _(k):
        peer = lax.rem(me + k, n)
        sum_copy(k, peer, peer).wait_recv()

    all_sums = jnp.sum(sums[...], axis=0)
    t_s, t_t, r_s, r_t = [all_sums[:, i : i + 1] for i in range(4)]
    omega = t_s / t_t
    rho_next = r_s - omega * r_t
    beta = rho_next / rho_start * (alpha / omega)
    sol = alpha * r_vec + omega * half_step
    res = half_step - omega * half_image
    direction = res + beta * (r_vec - omega * p_vec)
    for i, val in enumerate((sol, res, direction)):
        for p in range(2):
            out_ref[i, :, p, :] = val[p * S : (p + 1) * S, 0:C]

    @pl.loop(1, n)
    def _(k):
        sum_copy(k, me, lax.rem(me + k, n)).wait_send()


def solution(mesh):
    n = mesh.shape["sph"]

    def on_device(
        right_side, positions, sphere_radii, azimuths, pair_flags, pair_counts, tilt_matrix, axial_terms
    ):
        S, _, C = right_side.shape
        CP = -(-C // LANES) * LANES
        terms = axial_terms.shape[0]
        total = pair_flags.shape[1]
        q = n // 8
        table = orders_table(C // 2)
        orders = np.zeros((1, CP), np.float32)
        orders[0, : C // 2] = table
        orders[0, C // 2 : C] = table
        vmem = pl.BlockSpec(memory_space=pltpu.VMEM)
        out = pltpu.VMEM((3,) + right_side.shape, F32)
        stacked = pl.pallas_call(
            functools.partial(kernel, n, S, C, CP, terms),
            out_shape=out,
            in_specs=[vmem] * 8 + [pl.BlockSpec(memory_space=pl.ANY)],
            out_specs=vmem,
            scratch_shapes=[
                pltpu.VMEM((8, LANES), F32),
                pltpu.VMEM((S, 2 * CP), F32),
                pltpu.VMEM((S, 2 * CP), F32),
                pltpu.VMEM((total, 2 * CP), F32),
                pltpu.VMEM((total, 2 * CP), F32),
                pltpu.VMEM((total, 2 * CP), BF),
                pltpu.VMEM((total, 2 * CP), BF),
                pltpu.VMEM((terms * S, total), BF),
                pltpu.VMEM((terms * S, total), BF),
                pltpu.VMEM((CP, CP), BF),
                pltpu.VMEM((CP, CP), BF),
                pltpu.VMEM((CP, CP), BF),
                pltpu.VMEM((CP, CP), BF),
                pltpu.VMEM((terms, C, C), F32),
                pltpu.VMEM((terms * CP, CP), BF),
                pltpu.VMEM((terms * CP, CP), BF),
                pltpu.VMEM((n, 1, LANES), F32),
                pltpu.SemaphoreType.DMA,
                pltpu.SemaphoreType.DMA((2, 8, q)),
                pltpu.SemaphoreType.DMA((2, n)),
                pltpu.SemaphoreType.DMA((n,)),
                pltpu.SemaphoreType.DMA((n,)),
            ],
            compiler_params=pltpu.CompilerParams(
                collective_id=0, has_side_effects=True, vmem_limit_bytes=60 * 1024 * 1024
            ),
        )(
            right_side,
            positions,
            sphere_radii.reshape(1, S),
            azimuths.reshape(1, S),
            pair_counts.reshape(1, S),
            pair_flags,
            jnp.asarray(orders),
            tilt_matrix,
            axial_terms,
        )
        return (stacked[0], stacked[1], stacked[2])

    in_specs = (
        P("sph", None, None),
        P(None, "sph"),
        P("sph"),
        P("sph"),
        P("sph", None),
        P("sph"),
        P(),
        P(),
    )
    out_specs = (P("sph", None, None), P("sph", None, None), P("sph", None, None))
    return jax.shard_map(
        on_device, mesh=mesh, in_specs=in_specs, out_specs=out_specs, check_vma=False
    )
```

```python
import functools

import jax
import jax.numpy as jnp
import numpy as np
from jax import lax
from jax.experimental import pallas as pl
from jax.experimental.pallas import tpu as pltpu
from jax.sharding import PartitionSpec as P

coupling = 0.25
wavenum = 2.5
phase_step = 0.9
dist_floor = 0.8

LANES = 128
MESH = pl.DeviceIdType.MESH
BF = jnp.bfloat16
F32 = jnp.float32

TREES = (
    (0, 0, 0, 0, 0, 4, 2, 3, 4, 8, 8, 3, 0, 12, 2, 12),
    (4, 0, 0, 0, 4, 4, 4, 4, 4, 8, 8, 10, 8, 9, 12, 7),
)
RANKS = (
    (5, 2, 5, 8, 6, 11, 4, 9, 11, 3, 4, 4, 8, 15, 13, 6),
    (8, 10, 2, 4, 12, 3, 1, 8, 2, 11, 0, 7, 7, 13, 7, 0),
)
ORDERS = (
    (1, 2, 4, 3, 12, 8, 6, 5, 7, 14, 10, 13, 9, 11, 15),
    (0, 5, 6, 8, 7, 2, 10, 12, 1, 9, 14, 11, 13, 15, 3),
)


def children(kind, node):
    found = [i for i in range(16) if i != 4 * kind and TREES[kind][i] == node]
    return sorted(found, key=lambda i: RANKS[kind][i])


def route(q):
    if q != 4:
        firsts = [(1, 0), (2, 0), (3, 0)] + [(0, k) for k in range(1, q)]
        takes = []
        for k in range(q):
            if k + 1 < q:
                takes.append(((0, k + 1), [(1, k + 1), (2, k + 1), (3, k + 1)]))
            takes += [((ab, k), []) for ab in (1, 2, 3)]
        return [(firsts, takes)]
    kinds = []
    for own in range(2):
        firsts = [(k % 4, k // 4) for k in children(own, 4 * own)]
        takes = []
        for source in ORDERS[own]:
            ab, z = source % 4, source // 4
            kind = min(z, 3 - z)
            node = ab + 4 * (own if z < 2 else 3 - own)
            nexts = [
                ((k % 4) ^ ab, k // 4 if z < 2 else 3 - k // 4)
                for k in children(kind, node)
            ]
            takes.append(((ab, z), nexts))
        kinds.append((firsts, takes))
    return kinds


def orders_table(half):
    degree, orders = 1, []
    while len(orders) < half:
        orders += list(range(-degree, degree + 1))
        degree += 1
    return np.asarray(orders, np.float32)


def split(value):
    high = value.astype(BF)
    return high, (value - high.astype(F32)).astype(BF)


def dot3(high, low, w_high, w_low):
    rows = high.shape[0]
    both = jnp.dot(
        jnp.concatenate([high, low], axis=0), w_high, preferred_element_type=F32
    )
    return (
        both[:rows]
        + both[rows:]
        + jnp.dot(high, w_low, preferred_element_type=F32)
    )


def kernel(
    n, S, C, CP, terms,
    r_ref, pos_ref, rad_ref, az_ref, counts_ref, flags_ref, orders_ref, tilt_ref, axial_ref,
    out_ref,
    r_v, t_raw, flags_v, rows_own, rows_oth, r_own, r_oth,
    own1, own2, buf1, buf2, f_hi, f_lo, w_all, acc,
    t_hi, t_lo, tt_hi, tt_lo, gg_hi, gg_lo, g_raw, g_hi, g_lo,
    p_scr, q_scr, p_fin, q_fin, part_own, part_oth, s3, t3, p3, sums,
    in_sem, send_sem, recv_sem, pair_send, pair_recv, sum_send, sum_recv,
):
    half = C // 2
    q = n // 8
    S2 = 2 * S
    PL = 8 * S
    kinds = route(q)
    me = lax.axis_index("sph")
    core = lax.rem(me, 2)
    x_bit = lax.rem(me // 2, 2)
    y_bit = lax.rem(me // 4, 2)
    z_at = me // 8
    chip = me - core
    other = chip + 1 - core
    chip_x = chip + 2 - 4 * x_bit
    chip_y = chip + 4 - 8 * y_bit
    chip_d = chip_x + chip_y - chip

    if q == 4:
        mirror = z_at // 2
        at_end = (z_at + mirror * (3 - 2 * z_at)) == 0
        conds = [at_end, jnp.logical_not(at_end)]

        def place(k):
            return k + mirror * (3 - 2 * k)
    else:
        conds = [None]

        def place(k):
            at, bit = z_at, 1
            while bit <= k:
                if k & bit:
                    at = at + bit - 2 * bit * lax.rem(z_at // bit, 2)
                bit *= 2
            return at

    def pick(values):
        if len(values) == 1:
            return values[0]
        return jnp.where(at_end, values[0], values[1])

    def guarded(index, body):
        if conds[index] is None:
            body()
        else:
            pl.when(conds[index])(body)

    chip_a = chip_x * (1 - core) + chip_y * core
    chip_b = chip_y * (1 - core) + chip_x * core
    own_bases = (chip, chip_a, chip_b, chip_d)
    pol_bases = ((chip, chip_x, chip_y, chip_d), (chip, chip_y, chip_x, chip_d))

    def chip_at(bases, where):
        return bases[where[0]] + 8 * (place(where[1]) - z_at)

    barrier = pltpu.get_barrier_semaphore()
    line = [chip_at(own_bases, (0, k)) for k in range(q)] if q != 4 else None
    if q == 4:
        line = [chip + 8 * (lax.rem(z_at + k, q) - z_at) for k in range(1, q)]
    else:
        line = line[1:]
    peers = [other]
    for base in [chip_x, chip_y, chip_d] + line:
        peers += [base, base + 1]
    for peer in peers:
        pl.semaphore_signal(barrier, inc=1, device_id=(peer,), device_id_type=MESH)

    core_rows = pl.ds(pl.multiple_of(core * S, S), S)
    other_rows = pl.ds(pl.multiple_of((1 - core) * S, S), S)
    r_copy = pltpu.make_async_copy(r_ref, r_v, in_sem.at[0])
    t_copy = pltpu.make_async_copy(tilt_ref, t_raw, in_sem.at[1])
    f_copy = pltpu.make_async_copy(flags_ref, flags_v.at[core_rows, :], in_sem.at[2])
    g_copy = pltpu.make_async_copy(axial_ref, g_raw, in_sem.at[3])
    for copy in (r_copy, t_copy, f_copy, g_copy):
        copy.start()

    rows_own[...] = jnp.zeros_like(rows_own)
    rows_own[0:3, 0:S] = pos_ref[...]
    rows_own[3:4, 0:S] = rad_ref[...]
    rows_own[4:5, 0:S] = az_ref[...]
    rows_own[5:6, 0:S] = counts_ref[...].astype(F32)
    cols = rows_own[...].T[0:S]
    lane = lax.broadcasted_iota(jnp.int32, (S, CP), 1)
    lane2 = lax.broadcasted_iota(jnp.int32, (S2, CP), 1)

    def swapped(v):
        return jnp.where(
            lane2 < half, -pltpu.roll(v, CP - half, 1), pltpu.roll(v, half, 1)
        )

    def padded(v):
        return jnp.concatenate([v, jnp.zeros((v.shape[0], CP - C), v.dtype)], axis=1)

    phases = cols[:, 4:5] * orders_ref[...]
    cos_o = jnp.cos(phases)
    sin_o = jnp.sin(phases)
    cos2 = jnp.concatenate([cos_o, cos_o], axis=0)
    sin2 = jnp.concatenate([sin_o, sin_o], axis=0)

    t_copy.wait()
    for ref in (t_hi, t_lo):
        ref[C:CP, :] = jnp.zeros((CP - C, CP), BF)
    th, tl = split(t_raw[...])
    t_hi[0:C, :] = padded(th)
    t_lo[0:C, :] = padded(tl)
    r_copy.wait()
    for p in range(2):
        r_own[p] = padded(r_v[:, p, :])
    r_vec = jnp.concatenate([r_own[0], r_own[1]], axis=0)
    turned = cos2 * r_vec + sin2 * swapped(r_vec)
    high, low = split(turned)
    framed = dot3(high, low, t_hi[...], t_lo[...])
    for p in range(2):
        block = framed[p * S : (p + 1) * S]
        for i in range(4):
            block = jnp.where(lane == C + i, cols[:, i : i + 1], block)
        own1[p] = block

    def chip_rows(origin):
        return pl.ds(pl.multiple_of(origin * S, S2), S2)

    def dev_rows(origin):
        return pl.ds(pl.multiple_of(origin * S, S), S)

    buf1[dev_rows(me), :] = own1[core]

    waits = [[] for _ in conds]
    loose = []

    def remote(src, dst, s_sem, r_sem, dev):
        return pltpu.make_async_remote_copy(
            src_ref=src, dst_ref=dst, send_sem=s_sem, recv_sem=r_sem,
            device_id=(dev,), device_id_type=MESH,
        )

    def pair_copy(i, src, dst):
        return remote(src, dst, pair_send.at[i], pair_recv.at[i], other)

    def pair_start(i, src, dst):
        copy = pair_copy(i, src, dst)
        copy.start()
        loose.append(copy)

    counters = {}

    def next_sem(phase, kind):
        i = counters.get((phase, kind), 0)
        counters[(phase, kind)] = i + 1
        return send_sem.at[phase, i]

    def dispatch(kind, copies):
        if not copies:
            return
        waits[kind].extend(copies)

        def body():
            for copy in copies:
                copy.start()

        guarded(kind, body)

    def first_sends(phase, buf):
        for kind, (firsts, _) in enumerate(kinds):
            copies = []
            for where in firsts:
                if phase == 0:
                    for p in range(2):
                        copies.append(
                            remote(
                                own1.at[p], buf.at[dev_rows(me), :],
                                next_sem(phase, kind), recv_sem.at[phase, chip // 2],
                                chip_at(pol_bases[p], where) + p,
                            )
                        )
                else:
                    copies.append(
                        remote(
                            own2, buf.at[chip_rows(chip), :],
                            next_sem(phase, kind), recv_sem.at[phase, chip // 2],
                            chip_at(own_bases, where) + core,
                        )
                    )
            dispatch(kind, copies)

    seen = []
    for firsts, takes in kinds:
        counts = {}
        done = []
        own_z = 0 if q != 4 else len(seen)
        counts[own_z] = 1
        for i, ((ab, z), _) in enumerate(takes):
            counts[z] = counts.get(z, 0) + 1
            if counts[z] == 4:
                done.append((z, i))
        seen.append(done)
    slot_of = [{z: s for s, (z, _) in enumerate(done)} for done in seen]
    ready = [max(done[s][1] for done in seen) for s in range(q)]

    def absorb(buf, origin, slot):
        at = pl.ds(pl.multiple_of(slot * PL + lax.rem(origin, 8) * S, S2), S2)
        high, low = split(buf[chip_rows(origin), :])
        f_hi[at, :] = high
        f_lo[at, :] = low

    def plane(slot):
        return pick([place(done[slot][0]) for done in seen])

    def gather_product(pair):
        k0 = 2 * PL * pair
        ks = slice(k0, k0 + 2 * PL)
        rows = terms * S2
        both = jnp.dot(w_all[:, ks], f_hi[ks, :], preferred_element_type=F32)
        total = (
            both[:rows]
            + both[rows:]
            + jnp.dot(w_all[0:rows, ks], f_lo[ks, :], preferred_element_type=F32)
        )
        if pair > 0:
            total = total + acc[...]
        if pair < q // 2 - 1:
            acc[...] = total
        return total

    def gather(phase, buf, fillers, on_plane):
        fillers = list(fillers)
        steps = len(kinds[0][1])
        gathered = None
        for i in range(steps):
            origin = pick([chip_at(own_bases, takes[i][0]) for _, takes in kinds])
            slot = pick([slot_of[j][takes[i][0][1]] for j, (_, takes) in enumerate(kinds)])
            ref = buf.at[chip_rows(origin), :]
            remote(
                ref, ref, send_sem.at[phase, 0], recv_sem.at[phase, origin // 2], other
            ).wait_recv()
            for kind, (_, takes) in enumerate(kinds):
                dispatch(
                    kind,
                    [
                        remote(
                            ref, ref, next_sem(phase, kind),
                            recv_sem.at[phase, origin // 2],
                            chip_at(own_bases, where) + core,
                        )
                        for where in takes[i][1]
                    ],
                )
            absorb(buf, origin, slot)
            if fillers:
                fillers.pop(0)()
            for s in range(q):
                if ready[s] == i:
                    if s == 0:
                        while fillers:
                            fillers.pop(0)()
                    on_plane(s)
                    if s % 2 == 1:
                        gathered = gather_product(s // 2)
        return gathered

    pl.semaphore_wait(barrier, len(peers))
    first_sends(0, buf1)
    pair_start(0, own1.at[1 - core], buf1.at[dev_rows(me), :])
    pair_start(1, rows_own, rows_oth)
    pair_start(2, r_own.at[1 - core], r_oth)
    f_copy.wait()
    pair_start(3, flags_v.at[core_rows, :], flags_v.at[core_rows, :])

    def pair_wait(i, ref):
        pair_copy(i, ref, ref).wait_recv()

    zeros_pad = jnp.zeros((CP - C, CP), BF)

    def fill_tilt():
        h2, l2 = split(t_raw[...].T)
        for ref, v in ((tt_hi, h2), (tt_lo, l2)):
            ref[0:C, :] = padded(v)
            ref[C:CP, :] = zeros_pad

    def fill_gram():
        h2, l2 = split(dot3(tt_hi[...], tt_lo[...], t_hi[...], t_lo[...]))
        gg_hi[...] = h2
        gg_lo[...] = l2

    def fill_axial(m):
        h2, l2 = split(g_raw[m])
        for ref, v in ((g_hi, h2), (g_lo, l2)):
            ref[m * CP : m * CP + C, :] = padded(v)
            ref[m * CP + C : (m + 1) * CP, :] = zeros_pad

    fill_tilt()
    g_copy.wait()
    pair_wait(1, rows_oth)
    cols_oth = rows_oth[...].T[0:S]
    first = core == 0
    cols2 = jnp.concatenate(
        [jnp.where(first, cols, cols_oth), jnp.where(first, cols_oth, cols)], axis=0
    )
    phases = cols2[:, 4:5] * orders_ref[...]
    cos_t = jnp.cos(phases)
    sin_t = jnp.sin(phases)
    root = 1.0 / jnp.sqrt(1.0 + cols2[:, 5:6])
    pair_wait(2, r_oth)
    r_mine = r_own[core]
    r32 = jnp.concatenate(
        [jnp.where(first, r_mine, r_oth[...]), jnp.where(first, r_oth[...], r_mine)], axis=0
    )
    pair_wait(3, flags_v.at[other_rows, :])
    pair_wait(0, buf1.at[dev_rows(other), :])
    own_slot = pick([slot_of[j][0 if q != 4 else j] for j in range(len(kinds))])
    absorb(buf1, chip, own_slot)

    at = C - (CP - LANES)

    def weights(s):
        z = plane(s)
        geo = buf1[pl.ds(pl.multiple_of(z * PL, PL), PL), CP - LANES :].T
        flags = flags_v[:, pl.ds(pl.multiple_of(z * PL, PL), PL)]
        dx = cols2[:, 0:1] - geo[at : at + 1]
        dy = cols2[:, 1:2] - geo[at + 1 : at + 2]
        dz = cols2[:, 2:3] - geo[at + 2 : at + 3]
        distance = jnp.sqrt(dx * dx + dy * dy + dz * dz)
        ratio = (cols2[:, 3:4] + geo[at + 3 : at + 4]) / jnp.maximum(distance, dist_floor)
        wave = wavenum * distance
        cos_w = coupling * jnp.cos(wave)
        sin_w = coupling * jnp.sin(wave)
        power = jnp.ones_like(distance)
        for m in range(terms):
            turn_c = float(np.cos(phase_step * m))
            turn_s = float(np.sin(phase_step * m))
            keep = (flags != 0) if m == 0 else (flags == 1)
            weight = jnp.where(keep, power * (turn_c * cos_w - turn_s * sin_w), 0.0)
            power = power * ratio
            high, low = split(weight)
            w_all[m * S2 : (m + 1) * S2, s * PL : (s + 1) * PL] = high
            w_all[(terms + m) * S2 : (terms + m + 1) * S2, s * PL : (s + 1) * PL] = low

    def couple(gathered):
        x = jnp.concatenate(
            [gathered[m * S2 : (m + 1) * S2] for m in range(terms)], axis=1
        )
        high, low = split(x)
        return dot3(high, low, g_hi[...], g_lo[...])

    def unframed(coupled):
        high, low = split(coupled)
        v = dot3(high, low, tt_hi[...], tt_lo[...]) * root
        return cos_t * v - sin_t * swapped(v)

    fillers = [functools.partial(fill_axial, m) for m in range(terms)] + [fill_gram]
    coupled = couple(gather(0, buf1, fillers, weights))

    framed = buf1[chip_rows(chip), :]
    high, low = split(coupled)
    block = framed - dot3(high, low, gg_hi[...], gg_lo[...]) * root
    r_r = jnp.sum(r32 * r32, axis=1, keepdims=True)
    r_p = r_r - root * jnp.sum(framed * coupled, axis=1, keepdims=True)
    block = jnp.where(lane2 == C, r_r, block)
    block = jnp.where(lane2 == C + 1, r_p, block)
    own2[...] = block
    first_sends(1, buf2)
    buf2[chip_rows(chip), :] = block
    absorb(buf2, chip, own_slot)

    p_vec = r32 - unframed(coupled)
    p_scr[...] = p_vec
    pair_start(4, p_scr.at[other_rows, :], p_fin.at[core])
    p_fin[core] = p_scr[core_rows, :]

    gathered = gather(1, buf2, [], lambda s: None)
    part_own[...] = jnp.broadcast_to(
        jnp.sum(buf2[:, CP - LANES :], axis=0, keepdims=True), part_own.shape
    )
    pair_start(5, part_own, part_oth)
    q_vec = p_vec - unframed(couple(gathered))
    q_scr[...] = q_vec
    pair_start(6, q_scr.at[other_rows, :], q_fin.at[core])
    q_fin[core] = q_scr[core_rows, :]

    pair_wait(5, part_oth)
    starts = part_own[0:1] + part_oth[0:1]
    rho_start = starts[:, at : at + 1]
    alpha = rho_start / starts[:, at + 1 : at + 2]
    half_step = r32 - alpha * p_vec
    half_image = p_vec - alpha * q_vec

    def total(a, b):
        return jnp.sum(jnp.sum(a * b, axis=0, keepdims=True), axis=1, keepdims=True)

    lane1 = lax.broadcasted_iota(jnp.int32, (1, LANES), 1)
    row = jnp.zeros((1, LANES), F32)
    pairs = (
        (half_image, half_step),
        (half_image, half_image),
        (r32, half_step),
        (r32, half_image),
    )
    for i, (a, b) in enumerate(pairs):
        row = jnp.where(lane1 == i, total(a, b), row)
    sums[me] = row

    def sum_copy(k, origin, dev):
        return remote(
            sums.at[origin], sums.at[origin], sum_send.at[k], sum_recv.at[origin], dev
        )

    @pl.loop(1, n)
    def _(k):
        sum_copy(k, me, lax.rem(me + k, n)).start()

    pair_wait(4, p_fin.at[1 - core])
    pair_wait(6, q_fin.at[1 - core])
    for p in range(2):
        p_p = p_fin[p]
        s3[:, p, :] = (r_own[p] - alpha * p_p)[:, 0:C]
        t3[:, p, :] = (p_p - alpha * q_fin[p])[:, 0:C]
        p3[:, p, :] = p_p[:, 0:C]

    for copy in loose:
        copy.wait_send()
    for kind, copies in enumerate(waits):

        def body(copies=copies):
            for copy in copies:
                copy.wait_send()

        guarded(kind, body)

    @pl.loop(1, n)
    def _(k):
        peer = lax.rem(me + k, n)
        sum_copy(k, peer, peer).wait_recv()

    all_sums = jnp.sum(sums[...], axis=0)
    t_s, t_t, r_s, r_t = [all_sums[:, i : i + 1] for i in range(4)]
    omega = t_s / t_t
    rho_next = r_s - omega * r_t
    beta = rho_next / rho_start * (alpha / omega)
    alpha = alpha.reshape(1, 1, 1)
    omega = omega.reshape(1, 1, 1)
    beta = beta.reshape(1, 1, 1)
    r_val = r_v[...]
    s_val = s3[...]
    res = s_val - omega * t3[...]
    out_ref[0] = alpha * r_val + omega * s_val
    out_ref[1] = res
    out_ref[2] = res + beta * (r_val - omega * p3[...])

    @pl.loop(1, n)
    def _(k):
        sum_copy(k, me, lax.rem(me + k, n)).wait_send()


def solution(mesh):
    n = mesh.shape["sph"]

    def on_device(
        right_side, positions, sphere_radii, azimuths, pair_flags, pair_counts, tilt_matrix, axial_terms
    ):
        S, _, C = right_side.shape
        CP = -(-C // LANES) * LANES
        terms = axial_terms.shape[0]
        total = pair_flags.shape[1]
        q = n // 8
        most = max(
            2 * len(firsts) + sum(len(nexts) for _, nexts in takes)
            for firsts, takes in route(q)
        )
        table = orders_table(C // 2)
        orders = np.zeros((1, CP), np.float32)
        orders[0, : C // 2] = table
        orders[0, C // 2 : C] = table
        vmem = pl.BlockSpec(memory_space=pltpu.VMEM)
        anywhere = pl.BlockSpec(memory_space=pl.ANY)
        out = pltpu.VMEM((3,) + right_side.shape, F32)
        stacked = pl.pallas_call(
            functools.partial(kernel, n, S, C, CP, terms),
            out_shape=out,
            in_specs=[anywhere, vmem, vmem, vmem, vmem, anywhere, vmem, anywhere, anywhere],
            out_specs=vmem,
            scratch_shapes=[
                pltpu.VMEM((S, 2, C), F32),
                pltpu.VMEM((C, C), F32),
                pltpu.VMEM((2 * S, total), jnp.int32),
                pltpu.VMEM((8, LANES), F32),
                pltpu.VMEM((8, LANES), F32),
                pltpu.VMEM((2, S, CP), F32),
                pltpu.VMEM((S, CP), F32),
                pltpu.VMEM((2, S, CP), F32),
                pltpu.VMEM((2 * S, CP), F32),
                pltpu.VMEM((total, CP), F32),
                pltpu.VMEM((total, CP), F32),
                pltpu.VMEM((total, CP), BF),
                pltpu.VMEM((total, CP), BF),
                pltpu.VMEM((4 * terms * S, total), BF),
                pltpu.VMEM((2 * terms * S, CP), F32),
                pltpu.VMEM((CP, CP), BF),
                pltpu.VMEM((CP, CP), BF),
                pltpu.VMEM((CP, CP), BF),
                pltpu.VMEM((CP, CP), BF),
                pltpu.VMEM((CP, CP), BF),
                pltpu.VMEM((CP, CP), BF),
                pltpu.VMEM((terms, C, C), F32),
                pltpu.VMEM((terms * CP, CP), BF),
                pltpu.VMEM((terms * CP, CP), BF),
                pltpu.VMEM((2 * S, CP), F32),
                pltpu.VMEM((2 * S, CP), F32),
                pltpu.VMEM((2, S, CP), F32),
                pltpu.VMEM((2, S, CP), F32),
                pltpu.VMEM((8, LANES), F32),
                pltpu.VMEM((8, LANES), F32),
                pltpu.VMEM((S, 2, C), F32),
                pltpu.VMEM((S, 2, C), F32),
                pltpu.VMEM((S, 2, C), F32),
                pltpu.VMEM((n, 1, LANES), F32),
                pltpu.SemaphoreType.DMA((4,)),
                pltpu.SemaphoreType.DMA((2, most)),
                pltpu.SemaphoreType.DMA((2, n // 2)),
                pltpu.SemaphoreType.DMA((7,)),
                pltpu.SemaphoreType.DMA((7,)),
                pltpu.SemaphoreType.DMA((n,)),
                pltpu.SemaphoreType.DMA((n,)),
            ],
            compiler_params=pltpu.CompilerParams(
                collective_id=0, has_side_effects=True, vmem_limit_bytes=60 * 1024 * 1024
            ),
        )(
            right_side,
            positions,
            sphere_radii.reshape(1, S),
            azimuths.reshape(1, S),
            pair_counts.reshape(1, S),
            pair_flags,
            jnp.asarray(orders),
            tilt_matrix,
            axial_terms,
        )
        return (stacked[0], stacked[1], stacked[2])

    in_specs = (
        P("sph", None, None),
        P(None, "sph"),
        P("sph"),
        P("sph"),
        P("sph", None),
        P("sph"),
        P(),
        P(),
    )
    out_specs = (P("sph", None, None), P("sph", None, None), P("sph", None, None))
    return jax.shard_map(
        on_device, mesh=mesh, in_specs=in_specs, out_specs=out_specs, check_vma=False
    )
```

```python
import functools

import jax
import jax.numpy as jnp
import numpy as np
from jax import lax
from jax.experimental import pallas as pl
from jax.experimental.pallas import tpu as pltpu
from jax.sharding import PartitionSpec as P

coupling = 0.25
wavenum = 2.5
phase_step = 0.9
dist_floor = 0.8

LANES = 128
MESH = pl.DeviceIdType.MESH
BF = jnp.bfloat16
F32 = jnp.float32

TREES = (
    (0, 0, 0, 0, 0, 4, 2, 3, 4, 8, 8, 3, 0, 12, 2, 12),
    (4, 0, 0, 0, 4, 4, 4, 4, 4, 8, 8, 10, 8, 9, 12, 7),
)
RANKS = (
    (5, 2, 5, 8, 6, 11, 4, 9, 11, 3, 4, 4, 8, 15, 13, 6),
    (8, 10, 2, 4, 12, 3, 1, 8, 2, 11, 0, 7, 7, 13, 7, 0),
)
ORDERS = (
    (1, 2, 4, 3, 12, 8, 6, 5, 7, 14, 10, 13, 9, 11, 15),
    (0, 5, 6, 8, 7, 2, 10, 12, 9, 1, 14, 11, 13, 15, 3),
)


def children(kind, node):
    found = [i for i in range(16) if i != 4 * kind and TREES[kind][i] == node]
    return sorted(found, key=lambda i: RANKS[kind][i])


def route(q):
    if q != 4:
        firsts = [(1, 0), (2, 0), (3, 0)] + [(0, k) for k in range(1, q)]
        takes = []
        for k in range(q):
            if k + 1 < q:
                takes.append(((0, k + 1), [(1, k + 1), (2, k + 1), (3, k + 1)]))
            takes += [((ab, k), []) for ab in (1, 2, 3)]
        return [(firsts, takes)]
    kinds = []
    for own in range(2):
        firsts = [(k % 4, k // 4) for k in children(own, 4 * own)]
        takes = []
        for source in ORDERS[own]:
            ab, z = source % 4, source // 4
            kind = min(z, 3 - z)
            node = ab + 4 * (own if z < 2 else 3 - own)
            nexts = [
                ((k % 4) ^ ab, k // 4 if z < 2 else 3 - k // 4)
                for k in children(kind, node)
            ]
            takes.append(((ab, z), nexts))
        kinds.append((firsts, takes))
    return kinds


def orders_table(half):
    degree, orders = 1, []
    while len(orders) < half:
        orders += list(range(-degree, degree + 1))
        degree += 1
    return np.asarray(orders, np.float32)


def split(value):
    high = value.astype(BF)
    return high, (value - high.astype(F32)).astype(BF)


def dot3(high, low, w_high, w_low):
    rows = high.shape[0]
    both = jnp.dot(
        jnp.concatenate([high, low], axis=0), w_high, preferred_element_type=F32
    )
    return (
        both[:rows]
        + both[rows:]
        + jnp.dot(high, w_low, preferred_element_type=F32)
    )


def kernel(
    n, S, C, CP, terms,
    r_ref, pos_ref, rad_ref, az_ref, counts_ref, flags_ref, orders_ref, tilt_ref, axial_ref,
    out_ref,
    r_v, t_raw, pos_v, rad_v, az_v, counts_v, orders_v, flags_v, rows_own, rows_oth, r_own, r_oth,
    own1, own2, buf1, buf2, f_hi, f_lo, w_all, acc,
    t_hi, t_lo, tt_hi, tt_lo, gg_hi, gg_lo, g_raw, g_hi, g_lo,
    p_scr, q_scr, p_fin, q_fin, part_own, part_oth, s3, t3, p3, sums,
    in_sem, send_sem, recv_sem, pair_send, pair_recv, sum_send, sum_recv,
):
    half = C // 2
    q = n // 8
    S2 = 2 * S
    PL = 8 * S
    kinds = route(q)
    me = lax.axis_index("sph")
    core = lax.rem(me, 2)
    x_bit = lax.rem(me // 2, 2)
    y_bit = lax.rem(me // 4, 2)
    z_at = me // 8
    chip = me - core
    other = chip + 1 - core
    chip_x = chip + 2 - 4 * x_bit
    chip_y = chip + 4 - 8 * y_bit
    chip_d = chip_x + chip_y - chip

    if q == 4:
        mirror = z_at // 2
        at_end = (z_at + mirror * (3 - 2 * z_at)) == 0
        conds = [at_end, jnp.logical_not(at_end)]

        def place(k):
            return k + mirror * (3 - 2 * k)
    else:
        conds = [None]

        def place(k):
            at, bit = z_at, 1
            while bit <= k:
                if k & bit:
                    at = at + bit - 2 * bit * lax.rem(z_at // bit, 2)
                bit *= 2
            return at

    def pick(values):
        if len(values) == 1:
            return values[0]
        return jnp.where(at_end, values[0], values[1])

    def guarded(index, body):
        if conds[index] is None:
            body()
        else:
            pl.when(conds[index])(body)

    chip_a = chip_x * (1 - core) + chip_y * core
    chip_b = chip_y * (1 - core) + chip_x * core
    own_bases = (chip, chip_a, chip_b, chip_d)
    pol_bases = ((chip, chip_x, chip_y, chip_d), (chip, chip_y, chip_x, chip_d))

    def chip_at(bases, where):
        return bases[where[0]] + 8 * (place(where[1]) - z_at)

    barrier = pltpu.get_barrier_semaphore()
    line = [chip_at(own_bases, (0, k)) for k in range(q)] if q != 4 else None
    if q == 4:
        line = [chip + 8 * (lax.rem(z_at + k, q) - z_at) for k in range(1, q)]
    else:
        line = line[1:]
    peers = [other]
    for base in [chip_x, chip_y, chip_d] + line:
        peers += [base, base + 1]
    for peer in peers:
        pl.semaphore_signal(barrier, inc=1, device_id=(peer,), device_id_type=MESH)

    core_rows = pl.ds(pl.multiple_of(core * S, S), S)
    other_rows = pl.ds(pl.multiple_of((1 - core) * S, S), S)
    r_copy = pltpu.make_async_copy(r_ref, r_v, in_sem.at[0])
    t_copy = pltpu.make_async_copy(tilt_ref, t_raw, in_sem.at[1])
    f_copy = pltpu.make_async_copy(flags_ref, flags_v.at[core_rows, :], in_sem.at[2])
    g_copy = pltpu.make_async_copy(axial_ref, g_raw, in_sem.at[3])
    small = [
        pltpu.make_async_copy(ref, dst, in_sem.at[4 + i])
        for i, (ref, dst) in enumerate(
            (
                (pos_ref, pos_v), (rad_ref, rad_v), (az_ref, az_v),
                (counts_ref, counts_v), (orders_ref, orders_v),
            )
        )
    ]
    for copy in small + [r_copy, t_copy, f_copy, g_copy]:
        copy.start()

    rows_own[...] = jnp.zeros_like(rows_own)
    for copy in small:
        copy.wait()
    rows_own[0:3, 0:S] = pos_v[...]
    rows_own[3:4, 0:S] = rad_v[...]
    rows_own[4:5, 0:S] = az_v[...]
    rows_own[5:6, 0:S] = counts_v[...].astype(F32)
    cols = rows_own[...].T[0:S]
    lane = lax.broadcasted_iota(jnp.int32, (S, CP), 1)
    lane2 = lax.broadcasted_iota(jnp.int32, (S2, CP), 1)

    def swapped(v):
        return jnp.where(
            lane2 < half, -pltpu.roll(v, CP - half, 1), pltpu.roll(v, half, 1)
        )

    def padded(v):
        return jnp.concatenate([v, jnp.zeros((v.shape[0], CP - C), v.dtype)], axis=1)

    phases = cols[:, 4:5] * orders_v[...]
    cos_o = jnp.cos(phases)
    sin_o = jnp.sin(phases)
    cos2 = jnp.concatenate([cos_o, cos_o], axis=0)
    sin2 = jnp.concatenate([sin_o, sin_o], axis=0)

    t_copy.wait()
    for ref in (t_hi, t_lo):
        ref[C:CP, :] = jnp.zeros((CP - C, CP), BF)
    th, tl = split(t_raw[...])
    t_hi[0:C, :] = padded(th)
    t_lo[0:C, :] = padded(tl)
    r_copy.wait()
    for p in range(2):
        r_own[p] = padded(r_v[:, p, :])
    r_vec = jnp.concatenate([r_own[0], r_own[1]], axis=0)
    turned = cos2 * r_vec + sin2 * swapped(r_vec)
    high, low = split(turned)
    framed = dot3(high, low, t_hi[...], t_lo[...])
    for p in range(2):
        block = framed[p * S : (p + 1) * S]
        for i in range(4):
            block = jnp.where(lane == C + i, cols[:, i : i + 1], block)
        own1[p] = block

    def chip_rows(origin):
        return pl.ds(pl.multiple_of(origin * S, S2), S2)

    def dev_rows(origin):
        return pl.ds(pl.multiple_of(origin * S, S), S)

    buf1[dev_rows(me), :] = own1[core]

    waits = [[] for _ in conds]
    loose = []

    def remote(src, dst, s_sem, r_sem, dev):
        return pltpu.make_async_remote_copy(
            src_ref=src, dst_ref=dst, send_sem=s_sem, recv_sem=r_sem,
            device_id=(dev,), device_id_type=MESH,
        )

    def pair_copy(i, src, dst):
        return remote(src, dst, pair_send.at[i], pair_recv.at[i], other)

    def pair_start(i, src, dst):
        copy = pair_copy(i, src, dst)
        copy.start()
        loose.append(copy)

    counters = {}

    def next_sem(phase, kind):
        i = counters.get((phase, kind), 0)
        counters[(phase, kind)] = i + 1
        return send_sem.at[phase, i]

    def dispatch(kind, copies):
        if not copies:
            return
        waits[kind].extend(copies)

        def body():
            for copy in copies:
                copy.start()

        guarded(kind, body)

    def first_sends(phase, buf):
        for kind, (firsts, _) in enumerate(kinds):
            copies = []
            for where in firsts:
                if phase == 0:
                    for p in range(2):
                        copies.append(
                            remote(
                                own1.at[p], buf.at[dev_rows(me), :],
                                next_sem(phase, kind), recv_sem.at[phase, chip // 2],
                                chip_at(pol_bases[p], where) + p,
                            )
                        )
                else:
                    copies.append(
                        remote(
                            own2, buf.at[chip_rows(chip), :],
                            next_sem(phase, kind), recv_sem.at[phase, chip // 2],
                            chip_at(own_bases, where) + core,
                        )
                    )
            dispatch(kind, copies)

    seen = []
    for firsts, takes in kinds:
        counts = {}
        done = []
        own_z = 0 if q != 4 else len(seen)
        counts[own_z] = 1
        for i, ((ab, z), _) in enumerate(takes):
            counts[z] = counts.get(z, 0) + 1
            if counts[z] == 4:
                done.append((z, i))
        seen.append(done)
    slot_of = [{z: s for s, (z, _) in enumerate(done)} for done in seen]
    ready = [max(done[s][1] for done in seen) for s in range(q)]

    def absorb(buf, origin, slot):
        at = pl.ds(pl.multiple_of(slot * PL + lax.rem(origin, 8) * S, S2), S2)
        high, low = split(buf[chip_rows(origin), :])
        f_hi[at, :] = high
        f_lo[at, :] = low

    def plane(slot):
        return pick([place(done[slot][0]) for done in seen])

    def gather_product(pair):
        k0 = 2 * PL * pair
        ks = slice(k0, k0 + 2 * PL)
        rows = terms * S2
        both = jnp.dot(w_all[:, ks], f_hi[ks, :], preferred_element_type=F32)
        total = (
            both[:rows]
            + both[rows:]
            + jnp.dot(w_all[0:rows, ks], f_lo[ks, :], preferred_element_type=F32)
        )
        if pair > 0:
            total = total + acc[...]
        if pair < q // 2 - 1:
            acc[...] = total
        return total

    def gather(phase, buf, fillers, on_plane):
        steps = len(kinds[0][1])
        relays = [
            max([i for i, (_, nexts) in enumerate(takes) if nexts]) for _, takes in kinds
        ]
        calm = min(max(relays), steps - 1)
        gathered = None
        for i in range(steps):
            origin = pick([chip_at(own_bases, takes[i][0]) for _, takes in kinds])
            slot = pick([slot_of[j][takes[i][0][1]] for j, (_, takes) in enumerate(kinds)])
            ref = buf.at[chip_rows(origin), :]
            remote(
                ref, ref, send_sem.at[phase, 0], recv_sem.at[phase, origin // 2], other
            ).wait_recv()
            for kind, (_, takes) in enumerate(kinds):
                dispatch(
                    kind,
                    [
                        remote(
                            ref, ref, next_sem(phase, kind),
                            recv_sem.at[phase, origin // 2],
                            chip_at(own_bases, where) + core,
                        )
                        for where in takes[i][1]
                    ],
                )
            absorb(buf, origin, slot)
            if i == calm:
                for fill in fillers:
                    fill()
            for s in range(q):
                if max(ready[s], calm) == i:
                    on_plane(s)
                    if s % 2 == 1:
                        gathered = gather_product(s // 2)
        return gathered

    pl.semaphore_wait(barrier, len(peers))
    first_sends(0, buf1)
    pair_start(0, own1.at[1 - core], buf1.at[dev_rows(me), :])
    pair_start(1, rows_own, rows_oth)
    pair_start(2, r_own.at[1 - core], r_oth)
    f_copy.wait()
    pair_start(3, flags_v.at[core_rows, :], flags_v.at[core_rows, :])

    def pair_wait(i, ref):
        pair_copy(i, ref, ref).wait_recv()

    zeros_pad = jnp.zeros((CP - C, CP), BF)

    def fill_tilt():
        h2, l2 = split(t_raw[...].T)
        for ref, v in ((tt_hi, h2), (tt_lo, l2)):
            ref[0:C, :] = padded(v)
            ref[C:CP, :] = zeros_pad

    def fill_gram():
        h2, l2 = split(dot3(tt_hi[...], tt_lo[...], t_hi[...], t_lo[...]))
        gg_hi[...] = h2
        gg_lo[...] = l2

    def fill_axial(m):
        h2, l2 = split(g_raw[m])
        for ref, v in ((g_hi, h2), (g_lo, l2)):
            ref[m * CP : m * CP + C, :] = padded(v)
            ref[m * CP + C : (m + 1) * CP, :] = zeros_pad

    fill_tilt()
    pair_wait(1, rows_oth)
    cols_oth = rows_oth[...].T[0:S]
    first = core == 0
    cols2 = jnp.concatenate(
        [jnp.where(first, cols, cols_oth), jnp.where(first, cols_oth, cols)], axis=0
    )
    phases = cols2[:, 4:5] * orders_v[...]
    cos_t = jnp.cos(phases)
    sin_t = jnp.sin(phases)
    root = 1.0 / jnp.sqrt(1.0 + cols2[:, 5:6])
    pair_wait(2, r_oth)
    r_mine = r_own[core]
    r32 = jnp.concatenate(
        [jnp.where(first, r_mine, r_oth[...]), jnp.where(first, r_oth[...], r_mine)], axis=0
    )
    pair_wait(3, flags_v.at[other_rows, :])
    pair_wait(0, buf1.at[dev_rows(other), :])
    own_slot = pick([slot_of[j][0 if q != 4 else j] for j in range(len(kinds))])
    absorb(buf1, chip, own_slot)

    at = C - (CP - LANES)

    def weights(s):
        z = plane(s)
        geo = buf1[pl.ds(pl.multiple_of(z * PL, PL), PL), CP - LANES :].T
        flags = flags_v[:, pl.ds(pl.multiple_of(z * PL, PL), PL)]
        dx = cols2[:, 0:1] - geo[at : at + 1]
        dy = cols2[:, 1:2] - geo[at + 1 : at + 2]
        dz = cols2[:, 2:3] - geo[at + 2 : at + 3]
        distance = jnp.sqrt(dx * dx + dy * dy + dz * dz)
        ratio = (cols2[:, 3:4] + geo[at + 3 : at + 4]) / jnp.maximum(distance, dist_floor)
        wave = wavenum * distance
        cos_w = coupling * jnp.cos(wave)
        sin_w = coupling * jnp.sin(wave)
        power = jnp.ones_like(distance)
        for m in range(terms):
            turn_c = float(np.cos(phase_step * m))
            turn_s = float(np.sin(phase_step * m))
            keep = (flags != 0) if m == 0 else (flags == 1)
            weight = jnp.where(keep, power * (turn_c * cos_w - turn_s * sin_w), 0.0)
            power = power * ratio
            high, low = split(weight)
            w_all[m * S2 : (m + 1) * S2, s * PL : (s + 1) * PL] = high
            w_all[(terms + m) * S2 : (terms + m + 1) * S2, s * PL : (s + 1) * PL] = low

    def couple(gathered):
        x = jnp.concatenate(
            [gathered[m * S2 : (m + 1) * S2] for m in range(terms)], axis=1
        )
        high, low = split(x)
        return dot3(high, low, g_hi[...], g_lo[...])

    def unframed(coupled):
        high, low = split(coupled)
        v = dot3(high, low, tt_hi[...], tt_lo[...]) * root
        return cos_t * v - sin_t * swapped(v)

    early = terms - 2
    g_copy.wait()
    for m in range(early):
        fill_axial(m)
    fillers = [functools.partial(fill_axial, m) for m in range(early, terms)] + [fill_gram]
    coupled = couple(gather(0, buf1, fillers, weights))

    framed = buf1[chip_rows(chip), :]
    high, low = split(coupled)
    block = framed - dot3(high, low, gg_hi[...], gg_lo[...]) * root
    r_r = jnp.sum(r32 * r32, axis=1, keepdims=True)
    r_p = r_r - root * jnp.sum(framed * coupled, axis=1, keepdims=True)
    block = jnp.where(lane2 == C, r_r, block)
    block = jnp.where(lane2 == C + 1, r_p, block)
    own2[...] = block
    first_sends(1, buf2)
    buf2[chip_rows(chip), :] = block
    absorb(buf2, chip, own_slot)

    p_vec = r32 - unframed(coupled)
    p_scr[...] = p_vec
    pair_start(4, p_scr.at[other_rows, :], p_fin.at[core])
    p_fin[core] = p_scr[core_rows, :]

    gathered = gather(1, buf2, [], lambda s: None)
    part_own[...] = jnp.broadcast_to(
        jnp.sum(buf2[:, CP - LANES :], axis=0, keepdims=True), part_own.shape
    )
    pair_start(5, part_own, part_oth)
    q_vec = p_vec - unframed(couple(gathered))
    q_scr[...] = q_vec
    pair_start(6, q_scr.at[other_rows, :], q_fin.at[core])
    q_fin[core] = q_scr[core_rows, :]

    pair_wait(5, part_oth)
    starts = part_own[0:1] + part_oth[0:1]
    rho_start = starts[:, at : at + 1]
    alpha = rho_start / starts[:, at + 1 : at + 2]
    half_step = r32 - alpha * p_vec
    half_image = p_vec - alpha * q_vec

    def total(a, b):
        return jnp.sum(jnp.sum(a * b, axis=0, keepdims=True), axis=1, keepdims=True)

    lane1 = lax.broadcasted_iota(jnp.int32, (1, LANES), 1)
    row = jnp.zeros((1, LANES), F32)
    pairs = (
        (half_image, half_step),
        (half_image, half_image),
        (r32, half_step),
        (r32, half_image),
    )
    for i, (a, b) in enumerate(pairs):
        row = jnp.where(lane1 == i, total(a, b), row)
    sums[me] = row

    def sum_copy(rows, dev):
        return remote(sums.at[rows], sums.at[rows], sum_send, sum_recv, dev)

    def sum_start(k):
        away = k // 8
        dev = 8 * lax.rem(z_at + away, q) + lax.rem(me + k, 8)
        sum_copy(pl.ds(me, 1), dev).start()

    far = sorted(range(1, n), key=lambda k: (-min(k // 8, q - k // 8), k))
    if n <= 64:
        for k in far:
            sum_start(k)
    else:
        pl.loop(1, n)(sum_start)

    pair_wait(4, p_fin.at[1 - core])
    pair_wait(6, q_fin.at[1 - core])
    for p in range(2):
        p_p = p_fin[p]
        s3[:, p, :] = (r_own[p] - alpha * p_p)[:, 0:C]
        t3[:, p, :] = (p_p - alpha * q_fin[p])[:, 0:C]
        p3[:, p, :] = p_p[:, 0:C]

    for copy in loose:
        copy.wait_send()
    for kind, copies in enumerate(waits):

        def body(copies=copies):
            for copy in copies:
                copy.wait_send()

        guarded(kind, body)

    everyone = sum_copy(pl.ds(0, n - 1), other)
    everyone.wait_recv()
    everyone.wait_send()
    all_sums = jnp.sum(sums[...], axis=0)
    t_s, t_t, r_s, r_t = [all_sums[:, i : i + 1] for i in range(4)]
    omega = t_s / t_t
    rho_next = r_s - omega * r_t
    beta = rho_next / rho_start * (alpha / omega)
    alpha = alpha.reshape(1, 1, 1)
    omega = omega.reshape(1, 1, 1)
    beta = beta.reshape(1, 1, 1)
    r_val = r_v[...]
    s_val = s3[...]
    res = s_val - omega * t3[...]
    out_ref[0] = alpha * r_val + omega * s_val
    out_ref[1] = res
    out_ref[2] = res + beta * (r_val - omega * p3[...])


def solution(mesh):
    n = mesh.shape["sph"]

    def on_device(
        right_side, positions, sphere_radii, azimuths, pair_flags, pair_counts, tilt_matrix, axial_terms
    ):
        S, _, C = right_side.shape
        CP = -(-C // LANES) * LANES
        terms = axial_terms.shape[0]
        total = pair_flags.shape[1]
        q = n // 8
        most = max(
            2 * len(firsts) + sum(len(nexts) for _, nexts in takes)
            for firsts, takes in route(q)
        )
        table = orders_table(C // 2)
        orders = np.zeros((1, CP), np.float32)
        orders[0, : C // 2] = table
        orders[0, C // 2 : C] = table
        vmem = pl.BlockSpec(memory_space=pltpu.VMEM)
        anywhere = pl.BlockSpec(memory_space=pl.ANY)
        out = pltpu.VMEM((3,) + right_side.shape, F32)
        stacked = pl.pallas_call(
            functools.partial(kernel, n, S, C, CP, terms),
            out_shape=out,
            in_specs=[anywhere] * 9,
            out_specs=vmem,
            scratch_shapes=[
                pltpu.VMEM((S, 2, C), F32),
                pltpu.VMEM((C, C), F32),
                pltpu.VMEM(positions.shape, F32),
                pltpu.VMEM((1, S), F32),
                pltpu.VMEM((1, S), F32),
                pltpu.VMEM((1, S), jnp.int32),
                pltpu.VMEM((1, CP), F32),
                pltpu.VMEM((2 * S, total), jnp.int32),
                pltpu.VMEM((8, LANES), F32),
                pltpu.VMEM((8, LANES), F32),
                pltpu.VMEM((2, S, CP), F32),
                pltpu.VMEM((S, CP), F32),
                pltpu.VMEM((2, S, CP), F32),
                pltpu.VMEM((2 * S, CP), F32),
                pltpu.VMEM((total, CP), F32),
                pltpu.VMEM((total, CP), F32),
                pltpu.VMEM((total, CP), BF),
                pltpu.VMEM((total, CP), BF),
                pltpu.VMEM((4 * terms * S, total), BF),
                pltpu.VMEM((2 * terms * S, CP), F32),
                pltpu.VMEM((CP, CP), BF),
                pltpu.VMEM((CP, CP), BF),
                pltpu.VMEM((CP, CP), BF),
                pltpu.VMEM((CP, CP), BF),
                pltpu.VMEM((CP, CP), BF),
                pltpu.VMEM((CP, CP), BF),
                pltpu.VMEM((terms, C, C), F32),
                pltpu.VMEM((terms * CP, CP), BF),
                pltpu.VMEM((terms * CP, CP), BF),
                pltpu.VMEM((2 * S, CP), F32),
                pltpu.VMEM((2 * S, CP), F32),
                pltpu.VMEM((2, S, CP), F32),
                pltpu.VMEM((2, S, CP), F32),
                pltpu.VMEM((8, LANES), F32),
                pltpu.VMEM((8, LANES), F32),
                pltpu.VMEM((S, 2, C), F32),
                pltpu.VMEM((S, 2, C), F32),
                pltpu.VMEM((S, 2, C), F32),
                pltpu.VMEM((n, 1, LANES), F32),
                pltpu.SemaphoreType.DMA((9,)),
                pltpu.SemaphoreType.DMA((2, most)),
                pltpu.SemaphoreType.DMA((2, n // 2)),
                pltpu.SemaphoreType.DMA((7,)),
                pltpu.SemaphoreType.DMA((7,)),
                pltpu.SemaphoreType.DMA,
                pltpu.SemaphoreType.DMA,
            ],
            compiler_params=pltpu.CompilerParams(
                collective_id=0, has_side_effects=True, vmem_limit_bytes=60 * 1024 * 1024
            ),
        )(
            right_side,
            positions,
            sphere_radii.reshape(1, S),
            azimuths.reshape(1, S),
            pair_counts.reshape(1, S),
            pair_flags,
            jnp.asarray(orders),
            tilt_matrix,
            axial_terms,
        )
        return (stacked[0], stacked[1], stacked[2])

    in_specs = (
        P("sph", None, None),
        P(None, "sph"),
        P("sph"),
        P("sph"),
        P("sph", None),
        P("sph"),
        P(),
        P(),
    )
    out_specs = (P("sph", None, None), P("sph", None, None), P("sph", None, None))
    return jax.shard_map(
        on_device, mesh=mesh, in_specs=in_specs, out_specs=out_specs, check_vma=False
    )
```
